32 devices in a mesh: kv: 4 (over y, x), seq: 8 (over z, core).
Axes of the slice: x: 2, y: 2, z: 4, core: 2. Of those that a mesh axis runs over, the one named last changes fastest.
Arguments:
- queries: bfloat16 [2048, 16384], P('seq', 'kv'), may hold values from -24 to 24
- keys: bfloat16 [2048, 1024], P('seq', 'kv'), may hold values from -24 to 24
- values: bfloat16 [2048, 1024], P('seq', 'kv'), may hold values from -6 to 6
- query_map: float32 [128, 128, 64], P('kv'), may hold values from -4 to 4
- key_map: float32 [128, 128, 64], P('kv'), may hold values from -4 to 4
Outputs:
- grad_query_map: float32 [128, 128, 64], P(('kv', 'seq'))
- grad_key_map: float32 [128, 128, 64], P(('kv', 'seq'))
The draws below stay inside these ranges and needn't reach their ends.
All inputs are finite; a program needn't handle non-finite values.
Results may differ from the reference program's by a relative error of at most 0.00165.
Values may be sent and summed in bfloat16 or wider, within the bound.
A program may use at most 128 MiB of HBM per device.

```python
import jax
import jax.numpy as jnp
from jax import lax

HQ = 128
KVH = 8
HD = 128
FMAP = 64
LENGTH = 2048
GROUP = 16


def teacher_pair(key):
    queries = jax.random.normal(jax.random.fold_in(key, 11), (LENGTH, HQ * HD), jnp.float32)
    keys = jax.random.normal(jax.random.fold_in(key, 12), (LENGTH, KVH * HD), jnp.float32)
    return (jnp.clip(queries, -24.0, 24.0), jnp.clip(keys, -24.0, 24.0))


def draw_queries(key, part):
    return teacher_pair(key)[0].astype(jnp.bfloat16)


def draw_keys(key, part):
    return teacher_pair(key)[1].astype(jnp.bfloat16)


def map_weights(key, salt):
    weights = jax.random.normal(jax.random.fold_in(key, salt), (HQ, HD, FMAP), jnp.float32) * HD ** (-0.5)
    return jnp.clip(weights, -4.0, 4.0)


def draw_query_map(key, part):
    return map_weights(key, 21)


def draw_key_map(key, part):
    return map_weights(key, 22)


def level_of(key, extent, cuts, smallest, top_value):
    def one(dim, blocks):
        draws = jax.random.uniform(jax.random.fold_in(jax.random.fold_in(key, 6), dim), (blocks,), jnp.float32, smallest / len(cuts), top_value / len(cuts))
        return jnp.repeat(jnp.exp(draws), extent[dim] // blocks).reshape((-1,) + (1,) * (len(extent) - dim - 1))

    level = one(*cuts[0])
    for cut in cuts[1:]:
        level = level * one(*cut)
    return level


def noise(rng, dims, scale, reach, pieces=(), kind=jnp.bfloat16):
    drawn = jax.random.normal(rng, dims, jnp.float32) * scale
    if len(pieces) > 0:
        drawn = level_of(rng, dims, pieces, -0.22, 0.18) * drawn
    return jnp.clip(drawn, min=-reach, max=reach).astype(kind)


def setup_inputs(seed: int = 0) -> dict:
    arg_keys = jax.random.split(jax.random.key(seed), 6)
    queries = draw_queries(jax.random.fold_in(arg_keys[5], 71), 0)
    keys = draw_keys(jax.random.fold_in(arg_keys[5], 71), 0)
    values = noise(arg_keys[2], (LENGTH, KVH * HD), 1.0, 6.0, ((0, 8), (1, 4)))
    query_map = draw_query_map(jax.random.fold_in(arg_keys[5], 71), 0)
    key_map = draw_key_map(jax.random.fold_in(arg_keys[5], 71), 0)
    return {"queries": queries, "keys": keys, "values": values, "query_map": query_map, "key_map": key_map}


def block_size(count):
    return max((d for d in range(1, min(count, 512) + 1) if count % d == 0))

def feature(logits):
    return jnp.concatenate([jax.nn.softmax(logits, axis=-1), jax.nn.softmax(-logits, axis=-1)], axis=-1)

def reference(queries, keys, values, query_map, key_map):
    qblock = block_size(LENGTH)
    nblocks = LENGTH // qblock
    scale = 1.0 / HD ** 0.5
    hi = lax.Precision.HIGHEST
    positions = jnp.arange(LENGTH, dtype=jnp.int32)

    def per_group(group_id):
        qg = lax.dynamic_slice_in_dim(queries, group_id * GROUP * HD, GROUP * HD, 1).reshape(LENGTH, GROUP, HD)
        kg = lax.dynamic_slice_in_dim(keys, group_id * HD, HD, 1)
        vg = lax.dynamic_slice_in_dim(values, group_id * HD, HD, 1)
        wq = lax.dynamic_slice_in_dim(query_map, group_id * GROUP, GROUP, 0)
        wk = lax.dynamic_slice_in_dim(key_map, group_id * GROUP, GROUP, 0)
        kf = kg.astype(jnp.float32)
        vf = vg.astype(jnp.float32)

        def teacher_block(index):
            qb = lax.dynamic_slice_in_dim(qg, index * qblock, qblock, 0).astype(jnp.float32)
            scores = jnp.einsum('tjd,sd->jts', qb, kf, precision=hi) * scale
            qpos = index * qblock + jnp.arange(qblock, dtype=jnp.int32)
            allowed = positions[None, :] <= qpos[:, None]
            peak = lax.optimization_barrier(jnp.max(jnp.where(allowed[None], scores, -1e+30), axis=-1))
            probs = jnp.where(allowed[None], jnp.exp(scores - peak[..., None]), 0.0)
            total = lax.optimization_barrier(jnp.sum(probs, axis=-1))
            mixed = jnp.einsum('jts,sd->tjd', probs, vf, precision=hi)
            return (mixed / total.T[..., None]).astype(jnp.bfloat16)
        teacher = lax.map(teacher_block, jnp.arange(nblocks, dtype=jnp.int32)).reshape(LENGTH, GROUP, HD)
        target = teacher.astype(jnp.float32)

        def loss_of(wq_in, wk_in):
            fq = feature(jnp.einsum('tjd,jdf->tjf', qg.astype(jnp.float32), wq_in, precision=hi))
            fk = feature(jnp.einsum('sd,jdf->sjf', kf, wk_in, precision=hi))
            lower = (jnp.arange(qblock)[:, None] >= jnp.arange(qblock)[None, :]).astype(jnp.float32)

            def step(carry, index):
                state, norm_sum, loss = carry
                fqb = lax.dynamic_slice_in_dim(fq, index * qblock, qblock, 0)
                fkb = lax.dynamic_slice_in_dim(fk, index * qblock, qblock, 0)
                vb = lax.dynamic_slice_in_dim(vf, index * qblock, qblock, 0)
                ob = lax.dynamic_slice_in_dim(target, index * qblock, qblock, 0)
                attn = jnp.einsum('tjf,sjf->jts', fqb, fkb, precision=hi) * lower[None]
                numer = jnp.einsum('jts,sd->tjd', attn, vb, precision=hi) + jnp.einsum('tjf,jfd->tjd', fqb, state, precision=hi)
                denom = lax.optimization_barrier(jnp.sum(attn, axis=-1)).T + jnp.einsum('tjf,jf->tj', fqb, norm_sum, precision=hi)
                student = numer / denom[..., None]
                loss = loss + jnp.sum((student - ob) ** 2)
                state = state + jnp.einsum('sjf,sd->jfd', fkb, vb, precision=hi)
                norm_sum = norm_sum + lax.optimization_barrier(jnp.sum(fkb, axis=0))
                return ((state, norm_sum, loss), None)
            start = (jnp.zeros((GROUP, 2 * FMAP, HD), jnp.float32), jnp.zeros((GROUP, 2 * FMAP), jnp.float32), jnp.zeros((), jnp.float32))
            final, _ = lax.scan(step, start, jnp.arange(nblocks, dtype=jnp.int32))
            return final[2] / LENGTH
        _, pullback = jax.vjp(loss_of, wq, wk)
        grad_q, grad_k = pullback(jnp.ones((), jnp.float32))
        return (grad_q, grad_k)
    grads_q, grads_k = lax.map(per_group, jnp.arange(KVH, dtype=jnp.int32))
    return (grads_q.reshape(HQ, HD, FMAP), grads_k.reshape(HQ, HD, FMAP))
```

```python
import functools

import jax
import jax.numpy as jnp
from jax import lax
from jax.experimental import pallas as pl
from jax.experimental.pallas import tpu as pltpu
from jax.sharding import PartitionSpec as P

HD = 128
ONES = 16
F32 = jnp.float32
BF16 = jnp.bfloat16
LOG2E = 1.4426950408889634


def nn(a, b):
    return lax.dot_general(a, b, (((1,), (0,)), ((), ())), preferred_element_type=F32)


def nt(a, b):
    return lax.dot_general(a, b, (((1,), (1,)), ((), ())), preferred_element_type=F32)


def split(x):
    high = x.astype(BF16)
    return high, (x - high.astype(F32)).astype(BF16)


def cat(parts, axis):
    return jnp.concatenate(parts, axis=axis)


def feature(logits):
    first = jnp.exp(logits - jnp.max(logits, axis=0, keepdims=True))
    second = jnp.exp(jnp.min(logits, axis=0, keepdims=True) - logits)
    first = first * (1.0 / jnp.sum(first, axis=0, keepdims=True))
    second = second * (1.0 / jnp.sum(second, axis=0, keepdims=True))
    return cat([first, second], 0)


def feature_back(phi, dphi):
    width = phi.shape[0] // 2
    prod = phi * dphi
    one = prod[:width] - phi[:width] * jnp.sum(prod[:width], axis=0, keepdims=True)
    two = prod[width:] - phi[width:] * jnp.sum(prod[width:], axis=0, keepdims=True)
    return one - two


def teacher(c, chunk, q, k_ref, va_ref, lower):
    scale = LOG2E / HD**0.5
    if c < 8:
        scores = [nt(k_ref[j * chunk : (j + 1) * chunk, :], q) for j in range(c + 1)]
        scores[c] = jnp.where(lower, scores[c], -1e30)
        peak = functools.reduce(jnp.maximum, scores)
        peak = jnp.max(peak, axis=0, keepdims=True) * scale
        acc = None
        for j in range(c + 1):
            probs = jnp.exp2(scores[j] * scale - peak).astype(BF16)
            part = nn(va_ref[:, j * chunk : (j + 1) * chunk], probs)
            acc = part if acc is None else acc + part
    else:

        def step(scores, start, state):
            peak, acc = state
            new = jnp.maximum(peak, jnp.max(scores, axis=0, keepdims=True) * scale)
            probs = jnp.exp2(scores * scale - new).astype(BF16)
            part = nn(va_ref[:, pl.ds(start, chunk)], probs)
            return new, acc * jnp.exp2(peak - new) + part

        def body(j, state):
            start = pl.multiple_of(j * chunk, chunk)
            return step(nt(k_ref[pl.ds(start, chunk), :], q), start, state)

        state = (
            jnp.full((1, chunk), -1e30, F32),
            jnp.zeros((HD + ONES, chunk), F32),
        )
        state = lax.fori_loop(0, c, body, state)
        last = jnp.where(lower, nt(k_ref[c * chunk : (c + 1) * chunk, :], q), -1e30)
        acc = step(last, c * chunk, state)[1]
    return (acc[:HD] * (1.0 / acc[HD : HD + 1])).astype(BF16).astype(F32)


def kernel(
    chunk, pos_ref, q_ref, k_ref, v_ref, wq_ref, wk_ref, gq_ref, gk_ref,
    va_ref, fk_ref, dfk_ref, adj_ref, wgt_ref,
):
    length = q_ref.shape[0]
    blocks = length // chunk

    @pl.when(pl.program_id(0) == 0)
    def _():
        va_ref[HD:, :] = jnp.ones((ONES, length), BF16)
        for c in range(blocks):
            cols = slice(c * chunk, (c + 1) * chunk)
            va_ref[:HD, cols] = v_ref[cols, :].astype(F32).T.astype(BF16)

    src = lax.broadcasted_iota(jnp.int32, (chunk, chunk), 0)
    dst = lax.broadcasted_iota(jnp.int32, (chunk, chunk), 1)
    lower = src <= dst
    wq2 = cat(split(wq_ref[0].T), 1)
    wk2 = cat(split(wk_ref[0].T), 1)
    width = wq2.shape[0]
    gq = jnp.zeros((width, HD), F32)
    state = jnp.zeros((HD + ONES, 2 * width), F32)
    norm = jnp.zeros((2 * width, 1), F32)
    for c in range(blocks):
        cols = slice(c * chunk, (c + 1) * chunk)
        q = q_ref[cols, :]
        k = k_ref[cols, :]
        v = v_ref[cols, :]
        va = va_ref[:, cols]
        target = teacher(c, chunk, q, k_ref, va_ref, lower)
        fq = feature(nt(wq2, cat([q, q], 1)))
        fk = feature(nt(wk2, cat([k, k], 1)))
        fk_ref[:, cols] = fk
        fqh, fql = split(fq)
        fkh, fkl = split(fk)
        frh, frl = split(fk.T)
        attn = nn(cat([frh, frl, frh], 1), cat([fqh, fqh, fql], 0))
        ath, atl = split(jnp.where(lower, attn, 0.0))
        sth, stl = split(state)
        num = nn(
            cat([va, va, sth, stl, sth], 1), cat([ath, atl, fqh, fqh, fql], 0)
        )
        inv = 1.0 / num[HD : HD + 1]
        student = num[:HD] * inv
        grad = (2.0 / length) * (student - target)
        dnum = grad * inv
        dden = -jnp.sum(grad * student, axis=0, keepdims=True) * inv
        dnh, dnl = split(dnum)
        dattn = nn(cat([v, v], 1), cat([dnh, dnl], 0)) + dden
        dah, dal = split(jnp.where(lower, dattn, 0.0))
        srh, srl = split(state[:HD].T)
        dfq = nn(
            cat([fkh, fkl, fkh, srh, srl, srh], 1),
            cat([dah, dah, dal, dnh, dnh, dnl], 0),
        ) + norm * dden
        dql = cat(split(feature_back(fq, dfq)), 0)
        both = nn(dql, q)
        gq = gq + both[:width] + both[width:]
        dfk_ref[:, cols] = nt(cat([fqh, fql, fqh], 1), cat([dah, dah, dal], 1))
        adj_ref[c] = nt(cat([fqh, fql, fqh], 1), cat([dnh, dnh, dnl], 1))
        wgt_ref[c] = jnp.broadcast_to(
            jnp.sum(fq * dden, axis=1, keepdims=True), wgt_ref.shape[1:]
        )
        both = nn(va, cat([frh, frl], 1))
        state = state + both[:, : 2 * width] + both[:, 2 * width :]
        norm = norm + jnp.sum(fk, axis=1, keepdims=True)
    gq_ref[0] = gq.T

    gk = jnp.zeros((width, HD), F32)
    adj = jnp.zeros((2 * width, HD), F32)
    wgt = jnp.zeros((2 * width, 1), F32)
    for c in reversed(range(blocks)):
        cols = slice(c * chunk, (c + 1) * chunk)
        v = v_ref[cols, :]
        dfk = dfk_ref[:, cols] + nt(cat(split(adj), 1), cat([v, v], 1)) + wgt
        dkl = cat(split(feature_back(fk_ref[:, cols], dfk)), 0)
        both = nn(dkl, k_ref[cols, :])
        gk = gk + both[:width] + both[width:]
        adj = adj + adj_ref[c]
        wgt = wgt + wgt_ref[c][:, :1]
    gk_ref[0] = gk.T


def shards(devices, queries, keys, values, query_map, key_map):
    tok = queries.shape[0]
    heads_dev = queries.shape[1] // HD
    kv_dev = keys.shape[1] // HD
    group = heads_dev // kv_dev
    own = heads_dev // devices
    width = query_map.shape[2]
    length = tok * devices
    parts = []
    for d in range(devices):
        g = d * own // group
        parts.append(queries[:, d * own * HD : (d + 1) * own * HD])
        parts.append(keys[:, g * HD : (g + 1) * HD])
        parts.append(values[:, g * HD : (g + 1) * HD])
    packed = jnp.stack(
        [cat(parts[3 * d : 3 * d + 3], 1) for d in range(devices)], axis=0
    )
    held = lax.all_to_all(packed, "seq", 0, 0, tiled=True)
    held = held.reshape(length, (own + 2) * HD)
    position = lax.axis_index("seq").astype(jnp.int32).reshape(1)
    chunk = 256 if length % 256 == 0 else HD
    blocks = length // chunk
    weights = pl.BlockSpec((1, HD, width), lambda h, pos: (pos[0] * own + h, 0, 0))
    grads = pl.BlockSpec((1, HD, width), lambda h, pos: (h, 0, 0))
    gq, gk = pl.pallas_call(
        functools.partial(kernel, chunk),
        grid_spec=pltpu.PrefetchScalarGridSpec(
            num_scalar_prefetch=1,
            grid=(own,),
            in_specs=[
                pl.BlockSpec((length, HD), lambda h, pos: (0, h)),
                pl.BlockSpec((length, HD), lambda h, pos: (0, own)),
                pl.BlockSpec((length, HD), lambda h, pos: (0, own + 1)),
                weights,
                weights,
            ],
            out_specs=[grads, grads],
            scratch_shapes=[
                pltpu.VMEM((HD + ONES, length), BF16),
                pltpu.VMEM((2 * width, length), F32),
                pltpu.VMEM((2 * width, length), F32),
                pltpu.VMEM((blocks, 2 * width, HD), F32),
                pltpu.VMEM((blocks, 2 * width, HD), F32),
            ],
        ),
        out_shape=[jax.ShapeDtypeStruct((own, HD, width), F32)] * 2,
        compiler_params=pltpu.CompilerParams(
            dimension_semantics=("arbitrary",), vmem_limit_bytes=60 * 1024 * 1024
        ),
    )(position, held, held, held, query_map, key_map)
    return gq, gk


def solution(mesh):
    return jax.shard_map(
        functools.partial(shards, mesh.shape["seq"]),
        mesh=mesh,
        in_specs=(
            P("seq", "kv"),
            P("seq", "kv"),
            P("seq", "kv"),
            P("kv", None, None),
            P("kv", None, None),
        ),
        out_specs=(P(("kv", "seq"), None, None), P(("kv", "seq"), None, None)),
        check_vma=False,
    )
```

```python
import functools

import jax
import jax.numpy as jnp
from jax import lax
from jax.experimental import pallas as pl
from jax.experimental.pallas import tpu as pltpu
from jax.sharding import PartitionSpec as P

HD = 128
ONES = 16
F32 = jnp.float32
BF16 = jnp.bfloat16
LOG2E = 1.4426950408889634


def nn(a, b):
    return lax.dot_general(a, b, (((1,), (0,)), ((), ())), preferred_element_type=F32)


def nt(a, b):
    return lax.dot_general(a, b, (((1,), (1,)), ((), ())), preferred_element_type=F32)


def split(x):
    high = x.astype(BF16)
    return high, (x - high.astype(F32)).astype(BF16)


def cat(parts, axis):
    return jnp.concatenate(parts, axis=axis)


def feature(logits):
    first = jnp.exp(logits - jnp.max(logits, axis=0, keepdims=True))
    second = jnp.exp(jnp.min(logits, axis=0, keepdims=True) - logits)
    first = first * (1.0 / jnp.sum(first, axis=0, keepdims=True))
    second = second * (1.0 / jnp.sum(second, axis=0, keepdims=True))
    return cat([first, second], 0)


def feature_back(phi, dphi):
    width = phi.shape[0] // 2
    prod = phi * dphi
    one = prod[:width] - phi[:width] * jnp.sum(prod[:width], axis=0, keepdims=True)
    two = prod[width:] - phi[width:] * jnp.sum(prod[width:], axis=0, keepdims=True)
    return one - two


def teacher(c, chunk, q, k_ref, va_ref, lower):
    scale = LOG2E / HD**0.5
    if c < 8:
        scores = [nt(k_ref[j * chunk : (j + 1) * chunk, :], q) for j in range(c + 1)]
        scores[c] = jnp.where(lower, scores[c], -1e30)
        peak = functools.reduce(jnp.maximum, scores)
        peak = jnp.max(peak, axis=0, keepdims=True) * scale
        acc = None
        for j in range(c + 1):
            probs = jnp.exp2(scores[j] * scale - peak).astype(BF16)
            part = nn(va_ref[:, j * chunk : (j + 1) * chunk], probs)
            acc = part if acc is None else acc + part
    else:

        def step(scores, start, state):
            peak, acc = state
            new = jnp.maximum(peak, jnp.max(scores, axis=0, keepdims=True) * scale)
            probs = jnp.exp2(scores * scale - new).astype(BF16)
            part = nn(va_ref[:, pl.ds(start, chunk)], probs)
            return new, acc * jnp.exp2(peak - new) + part

        def body(j, state):
            start = pl.multiple_of(j * chunk, chunk)
            return step(nt(k_ref[pl.ds(start, chunk), :], q), start, state)

        state = (
            jnp.full((1, chunk), -1e30, F32),
            jnp.zeros((HD + ONES, chunk), F32),
        )
        state = lax.fori_loop(0, c, body, state)
        last = jnp.where(lower, nt(k_ref[c * chunk : (c + 1) * chunk, :], q), -1e30)
        acc = step(last, c * chunk, state)[1]
    return (acc[:HD] * (1.0 / acc[HD : HD + 1])).astype(BF16).astype(F32)


def kernel(
    chunk, pos_ref, q_ref, k_ref, v_ref, wq_ref, wk_ref, gq_ref, gk_ref,
    va_ref, fk_ref, dfk_ref, adj_ref, wgt_ref,
):
    length = q_ref.shape[0]
    blocks = length // chunk

    @pl.when(pl.program_id(0) == 0)
    def _():
        va_ref[HD:, :] = jnp.ones((ONES, length), BF16)
        for c in range(blocks):
            cols = slice(c * chunk, (c + 1) * chunk)
            va_ref[:HD, cols] = v_ref[cols, :].astype(F32).T.astype(BF16)

    src = lax.broadcasted_iota(jnp.int32, (chunk, chunk), 0)
    dst = lax.broadcasted_iota(jnp.int32, (chunk, chunk), 1)
    lower = src <= dst
    wq2 = cat(split(wq_ref[0]), 1)
    wk2 = cat(split(wk_ref[0]), 1)
    width = wq2.shape[0]
    gq = jnp.zeros((width, HD), F32)
    state = jnp.zeros((HD + ONES, 2 * width), F32)
    norm = jnp.zeros((2 * width, 1), F32)
    for c in range(blocks):
        cols = slice(c * chunk, (c + 1) * chunk)
        q = q_ref[cols, :]
        k = k_ref[cols, :]
        v = v_ref[cols, :]
        va = va_ref[:, cols]
        target = teacher(c, chunk, q, k_ref, va_ref, lower)
        fq = feature(nt(wq2, cat([q, q], 1)))
        fk = feature(nt(wk2, cat([k, k], 1)))
        fk_ref[:, cols] = fk
        fqh, fql = split(fq)
        fkh, fkl = split(fk)
        frh, frl = split(fk.T)
        attn = nn(cat([frh, frl, frh], 1), cat([fqh, fqh, fql], 0))
        ath, atl = split(jnp.where(lower, attn, 0.0))
        sth, stl = split(state)
        num = nn(
            cat([va, va, sth, stl, sth], 1), cat([ath, atl, fqh, fqh, fql], 0)
        )
        inv = 1.0 / num[HD : HD + 1]
        student = num[:HD] * inv
        grad = (2.0 / length) * (student - target)
        dnum = grad * inv
        dden = -jnp.sum(grad * student, axis=0, keepdims=True) * inv
        dnh, dnl = split(dnum)
        dattn = nn(cat([v, v], 1), cat([dnh, dnl], 0)) + dden
        dah, dal = split(jnp.where(lower, dattn, 0.0))
        srh, srl = split(state[:HD].T)
        dfq = nn(
            cat([fkh, fkl, fkh, srh, srl, srh], 1),
            cat([dah, dah, dal, dnh, dnh, dnl], 0),
        ) + norm * dden
        dql = cat(split(feature_back(fq, dfq)), 0)
        both = nn(dql, q)
        gq = gq + both[:width] + both[width:]
        dfk_ref[:, cols] = nt(cat([fqh, fql, fqh], 1), cat([dah, dah, dal], 1))
        adj_ref[c] = nt(cat([fqh, fql, fqh], 1), cat([dnh, dnh, dnl], 1))
        wgt_ref[c] = jnp.broadcast_to(
            jnp.sum(fq * dden, axis=1, keepdims=True), wgt_ref.shape[1:]
        )
        both = nn(va, cat([frh, frl], 1))
        state = state + both[:, : 2 * width] + both[:, 2 * width :]
        norm = norm + jnp.sum(fk, axis=1, keepdims=True)
    gq_ref[0] = gq

    gk = jnp.zeros((width, HD), F32)
    adj = jnp.zeros((2 * width, HD), F32)
    wgt = jnp.zeros((2 * width, 1), F32)
    for c in reversed(range(blocks)):
        cols = slice(c * chunk, (c + 1) * chunk)
        v = v_ref[cols, :]
        dfk = dfk_ref[:, cols] + nt(cat(split(adj), 1), cat([v, v], 1)) + wgt
        dkl = cat(split(feature_back(fk_ref[:, cols], dfk)), 0)
        both = nn(dkl, k_ref[cols, :])
        gk = gk + both[:width] + both[width:]
        adj = adj + adj_ref[c]
        wgt = wgt + wgt_ref[c][:, :1]
    gk_ref[0] = gk


def shards(devices, queries, keys, values, query_map, key_map):
    tok = queries.shape[0]
    heads_dev = queries.shape[1] // HD
    kv_dev = keys.shape[1] // HD
    group = heads_dev // kv_dev
    own = heads_dev // devices
    width = query_map.shape[2]
    length = tok * devices
    position = lax.axis_index("seq").astype(jnp.int32).reshape(1)
    chunk = 256 if length % 256 == 0 else HD
    blocks = length // chunk
    maps = (jnp.swapaxes(query_map, 1, 2), jnp.swapaxes(key_map, 1, 2))

    def pack(first, count, extra):
        def body(*refs):
            for i, ref in enumerate(refs[:-1]):
                start = count * HD + (i - 1) * HD if i else 0
                refs[-1][0, :, start : start + ref.shape[1]] = ref[...]

        columns = (count + len(extra)) * HD
        return pl.pallas_call(
            body,
            grid=(devices,),
            in_specs=[
                pl.BlockSpec(
                    (tok, count * HD), lambda d: (0, (d * own + first) // count)
                )
            ]
            + [pl.BlockSpec((tok, HD), lambda d: (0, d * own // group))] * len(extra),
            out_specs=pl.BlockSpec((1, tok, columns), lambda d: (d, 0, 0)),
            out_shape=jax.ShapeDtypeStruct((devices, tok, columns), BF16),
        )(queries, *extra)

    def send(packed):
        held = lax.all_to_all(packed, "seq", 0, 0, tiled=True)
        return held.reshape(length, packed.shape[2])

    def run(first, count, held, shared, base):
        weights = pl.BlockSpec(
            (1, width, HD), lambda h, pos: (pos[0] * own + first + h, 0, 0)
        )
        grads = pl.BlockSpec((1, width, HD), lambda h, pos: (h, 0, 0))
        return pl.pallas_call(
            functools.partial(kernel, chunk),
            grid_spec=pltpu.PrefetchScalarGridSpec(
                num_scalar_prefetch=1,
                grid=(count,),
                in_specs=[
                    pl.BlockSpec((length, HD), lambda h, pos: (0, h)),
                    pl.BlockSpec((length, HD), lambda h, pos: (0, base)),
                    pl.BlockSpec((length, HD), lambda h, pos: (0, base + 1)),
                    weights,
                    weights,
                ],
                out_specs=[grads, grads],
                scratch_shapes=[
                    pltpu.VMEM((HD + ONES, length), BF16),
                    pltpu.VMEM((2 * width, length), F32),
                    pltpu.VMEM((2 * width, length), F32),
                    pltpu.VMEM((blocks, 2 * width, HD), F32),
                    pltpu.VMEM((blocks, 2 * width, HD), F32),
                ],
            ),
            out_shape=[jax.ShapeDtypeStruct((count, width, HD), F32)] * 2,
            compiler_params=pltpu.CompilerParams(
                dimension_semantics=("arbitrary",),
                vmem_limit_bytes=40 * 1024 * 1024,
            ),
        )(position, held, shared, shared, *maps)

    count = own // 2 if own % 2 == 0 else own
    shared = send(pack(0, count, (keys, values)))
    grads = [run(0, count, shared, shared, count)]
    if count < own:
        packed, shared = lax.optimization_barrier((pack(count, count, ()), shared))
        grads.append(run(count, count, send(packed), shared, count))
    gq, gk = (cat([g[i] for g in grads], 0) for i in range(2))
    return jnp.swapaxes(gq, 1, 2), jnp.swapaxes(gk, 1, 2)


def solution(mesh):
    return jax.shard_map(
        functools.partial(shards, mesh.shape["seq"]),
        mesh=mesh,
        in_specs=(
            P("seq", "kv"),
            P("seq", "kv"),
            P("seq", "kv"),
            P("kv", None, None),
            P("kv", None, None),
        ),
        out_specs=(P(("kv", "seq"), None, None), P(("kv", "seq"), None, None)),
        check_vma=False,
    )
```
